32 devices in a mesh: row: 4 (over y, core), col: 8 (over z, x).
Axes of the slice: x: 2, y: 2, z: 4, core: 2. Of those that a mesh axis runs over, the one named last changes fastest.
Arguments:
- rhs: bfloat16 [6144, 6144], P('row', 'col'), may hold values from -6 to 6
- basis_left: bfloat16 [6144, 6144], P('col', 'row'), may hold values from -1 to 1, as said below
- basis_right: bfloat16 [6144, 6144], P('row', 'col'), may hold values from -1 to 1, as said below
- eig_left: float32 [6144], P('row'), may hold values from 0.1 to 4
- eig_right: float32 [6144], P('col'), may hold values from 0.1 to 4
Outputs:
- solution: bfloat16 [6144, 6144], P('col', 'row')
The draws below stay inside these ranges and needn't reach their ends.
Inputs may be any that keep to these rules, and one draw needn't show every extreme that they name: `basis_left`: an orthogonal matrix drawn uniformly, rounded to bfloat16. `basis_right`: an orthogonal matrix drawn uniformly, rounded to bfloat16.
All inputs are finite; a program needn't handle non-finite values.
Results may differ from the reference program's by a relative error of at most 0.0085.
Values may be sent and summed in bfloat16 or wider, within the bound.
A program may use at most 128 MiB of HBM per device.

```python
import math
import jax
import jax.numpy as jnp

N = 6144


def orthogonal_matrix(key):
    normal_draw = jax.random.normal(key, (N, N), jnp.float32)
    factor_q, factor_r = jnp.linalg.qr(normal_draw)
    signs = jnp.where(jnp.diagonal(factor_r) < 0.0, -1.0, 1.0).astype(jnp.float32)
    return (factor_q * signs[None, :]).astype(jnp.bfloat16)


def draw_basis_left(key, part):
    return orthogonal_matrix(jax.random.fold_in(key, 11))


def draw_basis_right(key, part):
    return orthogonal_matrix(jax.random.fold_in(key, 23))


def block_levels(key, shape, pieces, smallest, top_value):
    level = 1.0
    for dim, parts in pieces:
        steps = jax.random.uniform(jax.random.fold_in(jax.random.fold_in(key, 6), dim), (parts,), jnp.float32, smallest / len(pieces), top_value / len(pieces))
        level = level * jnp.repeat(jnp.exp(steps), shape[dim] // parts).reshape((-1,) + (1,) * (len(shape) - 1 - dim))
    return level


def normal_values(own_key, extent, width, reach, cuts=(), kind=jnp.bfloat16):
    loudness = block_levels(own_key, extent, cuts, -0.22, 0.18) if cuts else 1.0
    array = jax.random.normal(own_key, extent, jnp.float32) * width * loudness
    return jnp.minimum(jnp.maximum(array, -reach), reach).astype(kind)


def setup_inputs(seed: int = 0) -> dict:
    key_list = jax.random.split(jax.random.key(seed), 6)
    return {
        "rhs": normal_values(key_list[0], (N, N), 1.0, 6.0, ((0, 4), (1, 8))),
        "basis_left": draw_basis_left(jax.random.fold_in(key_list[5], 71), 0),
        "basis_right": draw_basis_right(jax.random.fold_in(key_list[5], 71), 0),
        "eig_left": jnp.clip(jnp.exp(math.log(4.0) - 3.6888794 * jax.random.uniform(key_list[3], (N,), jnp.float32) ** block_levels(key_list[3], (N,), ((0, 4),), -0.2, 0.2)), 0.1, 4.0),
        "eig_right": jnp.clip(jnp.exp(math.log(4.0) - 3.6888794 * jax.random.uniform(key_list[4], (N,), jnp.float32) ** block_levels(key_list[4], (N,), ((0, 8),), -0.2, 0.2)), 0.1, 4.0),
    }


def reference(rhs, basis_left, basis_right, eig_left, eig_right):
    projected = jnp.dot(basis_left.T.astype(jnp.float32), rhs.astype(jnp.float32), preferred_element_type=jnp.float32).astype(jnp.bfloat16)
    second = jnp.dot(projected.astype(jnp.float32), basis_right.astype(jnp.float32), preferred_element_type=jnp.float32)
    scaled = (second / (eig_left[:, None] + eig_right[None, :])).astype(jnp.bfloat16)
    half = jnp.dot(basis_left.astype(jnp.float32), scaled.astype(jnp.float32), preferred_element_type=jnp.float32).astype(jnp.bfloat16)
    return jnp.dot(half.astype(jnp.float32), basis_right.T.astype(jnp.float32), preferred_element_type=jnp.float32).astype(jnp.bfloat16)
```

```python
import functools
import jax
import jax.numpy as jnp
from jax import lax
from jax.sharding import PartitionSpec as P

BF16, F32 = jnp.bfloat16, jnp.float32


def body(nz, nx, rhs, basis_left, basis_right, eig_left, eig_right):
    zg = [[z * nx + x for z in range(nz)] for x in range(nx)]
    x = lax.rem(lax.axis_index("col"), nx)
    row = lax.axis_index("row")
    step = rhs.shape[0] // nx

    def shift(a, s):
        if s % nx == 0:
            return a
        return lax.ppermute(a, "col", [(z * nx + i, z * nx + (i + s) % nx) for z in range(nz) for i in range(nx)])

    def sub(a, i):
        return lax.dynamic_slice_in_dim(a, i * step, step, axis=0)

    def row_gather(a):
        out = jnp.zeros((nz * a.shape[0], a.shape[1]), a.dtype)
        for r in range(nz):
            b = a if r == 0 else lax.ppermute(a, "row", [(i, (i + r) % nz) for i in range(nz)])
            out = lax.dynamic_update_slice_in_dim(out, b, lax.rem(row - r + nz, nz) * a.shape[0], axis=0)
        return out

    def own_sum(parts):
        total = parts[0]
        for s in range(1, nx):
            total = total + shift(parts[s].astype(BF16), -s).astype(F32)
        return total

    left = lax.all_gather(basis_left, "col", axis=0, tiled=True, axis_index_groups=zg)
    c_sub = [row_gather(shift(sub(rhs, lax.rem(x + s, nx)), s)) for s in range(nx)]
    right = [shift(basis_right, s) for s in range(nx)]
    right_sub = [lax.all_gather(sub(b, x), "row", axis=0, tiled=True) for b in right]

    projected = own_sum(
        [lax.dot_general(left, c, (((0,), (0,)), ((), ())), preferred_element_type=F32) for c in c_sub]
    ).astype(BF16)
    projected_all = lax.all_gather(projected, "col", axis=1, tiled=True, axis_index_groups=zg)
    second = own_sum([jnp.dot(projected_all, b, preferred_element_type=F32) for b in right_sub])
    scaled = (second / (eig_left[:, None] + eig_right[None, :])).astype(BF16)

    total = None
    for s in range(nx):
        part = jnp.dot(left, shift(scaled, s), preferred_element_type=F32).astype(BF16)
        half = lax.psum_scatter(part, "row", scatter_dimension=0, tiled=True)
        half = lax.all_gather(half, "row", axis=0, tiled=True)
        term = lax.dot_general(half, right[s], (((1,), (1,)), ((), ())), preferred_element_type=F32)
        total = term if total is None else total + term
    return lax.psum_scatter(total.astype(BF16), "col", scatter_dimension=0, tiled=True, axis_index_groups=zg)


def solution(mesh):
    nz = mesh.shape["row"]
    nx = mesh.shape["col"] // nz
    in_specs = (P("row", "col"), P("col", "row"), P("row", "col"), P("row"), P("col"))
    fn = functools.partial(body, nz, nx)
    return jax.shard_map(fn, mesh=mesh, in_specs=in_specs, out_specs=P("col", "row"), check_vma=False)
```
